32 devices in a mesh: rows: 8 (over y, x, core), cols: 4 (over z).
Axes of the slice: x: 2, y: 2, z: 4, core: 2. Of those that a mesh axis runs over, the one named last changes fastest.
Arguments:
- fmap1: bfloat16 [2, 256, 256, 256], P(None, 'rows', 'cols'), may hold values from -6 to 6
- fmap2: bfloat16 [2, 256, 256, 256], P(None, 'rows', 'cols'), may hold values from -6 to 6
- target_owner: int32 [2, 2048, 1], P(None, ('rows', 'cols')), may hold values from 0 to 31; in each aligned block of 64 rows (0 to 63, 64 to 127, ..., all dimensions but the last counted through in order) at most 4 rows name the same one
- target_tile: int32 [2, 2048], P(None, ('rows', 'cols')), may hold values from 0 to 31
Outputs:
- corr: float32 [2, 81, 131072], P(None, None, ('rows', 'cols'))
The draws below stay inside these ranges and needn't reach their ends.
Inputs may be any that keep to these rules, and one draw needn't show every extreme that they name: `target_owner`: at each level, the 64 query blocks of one region (aligned blocks of rows) name any one owner at most 4 times, a bound that some block reaches. `target_tile`: tile of the owner's region in the query block's frame, numbered row-major; level l uses it modulo that level's tile count.
All inputs are finite; a program needn't handle non-finite values.
Results may differ from the reference program's by a relative error of at most 0.0013.
Values may be sent and summed in bfloat16 or wider, within the bound.
A program may use at most 128 MiB of HBM per device.

```python
import math
import jax
import jax.numpy as jnp
import numpy as np
from jax import lax

C = 256
RADIUS = 4
LEVELS = 2
BATCH = 2
QH = 32
QW = 64
H0 = 256
W0 = 256
TILES = 32
QB_DEV = 64
CAP = 4
QBLK = 2048
N_ROWS = 8
N_COLS = 4


def with_ends(entries, stream_key, low, high):
    place = [jax.random.randint(jax.random.fold_in(stream_key, axis), (), 0, length) for axis, length in enumerate(entries.shape)]
    longest = entries.shape.index(max(entries.shape))
    neighbour = place[:longest] + [(place[longest] + 1) % entries.shape[longest]] + place[longest + 1:]
    return entries.at[tuple(place)].set(low).at[tuple(neighbour)].set(high)


def block_scale(key, extent, shards, low, largest):
    loudness, own = 1.0, jax.random.fold_in(key, 6)
    for axis_at, parts in shards:
        steps = jnp.exp(jax.random.uniform(jax.random.fold_in(own, axis_at), (parts,), jnp.float32, low / len(shards), largest / len(shards)))
        loudness = loudness * jnp.repeat(steps, extent[axis_at] // parts).reshape([-1 if axis == axis_at else 1 for axis in range(len(extent))])
    return loudness


def routed_block(own_key, own, number, rows, amount, top, reach, skew):
    order = jax.random.permutation(own_key, amount)
    packed, common = portions_of(amount, rows * top, reach, skew, True), portions_of(amount, rows * top, reach, skew, False)
    places = jnp.arange(amount)

    def named(tallies, offset_by):
        used = int((tallies > 0).sum())
        fixed = max(1, used // 4)
        passed = fixed + (places - fixed + offset_by * (used - fixed)) % max(1, amount - fixed)
        return jnp.zeros((amount,), jnp.int32).at[order[jnp.where(places < fixed, places, passed)]].set(jnp.asarray(tallies, jnp.int32))

    tallies = jnp.where(number % 4 == 0, named(packed, number // 4), named(common, number - number // 4 - 1))
    mixed = jax.random.permutation(jax.random.fold_in(own, 3), amount)
    source_of, receiver = mixed[0:amount // 2 * 2:2], mixed[1:amount // 2 * 2:2]
    margin = jnp.minimum(tallies[source_of] - 1, reach - tallies[receiver]) // 2
    margin = jnp.where((source_of == order[0]) | (receiver == order[0]) | (tallies[receiver] == 0), 0, jnp.maximum(margin, 0))
    passed = jax.random.randint(jax.random.fold_in(own, 4), (amount // 2,), 0, 1 << 20) % (margin + 1)
    tallies = tallies.at[source_of].add(-passed).at[receiver].add(passed)
    members = jnp.searchsorted(jnp.cumsum(tallies), jnp.arange(rows * top), side="right").astype(jnp.int32)
    table = members.reshape(top, rows).T
    table = table[jax.random.permutation(jax.random.fold_in(own, 1), rows)]
    offset_by = jax.random.randint(jax.random.fold_in(own, 2), (rows, 1), 0, top)
    return jnp.take_along_axis(table, (jnp.arange(top)[None, :] + offset_by) % top, axis=1)


def portions_of(number_of, total, reach, skew, full):
    weights = [(1 << 20) // math.isqrt(standing ** skew) + 1 for standing in range(1, number_of + 1)]
    largest = reach if full else min(reach, max(-(-total // number_of), total * weights[0] // sum(weights)))
    least = 1 if total - largest >= number_of - 1 else 0
    holding, rest = [largest] + [least] * (number_of - 1), total - largest - least * (number_of - 1)
    while rest > 0:
        candidates = [i for i in range(1, number_of) if holding[i] < largest] or [i for i in range(1, number_of) if holding[i] < reach]
        whole, remaining = sum([weights[i] for i in candidates]), rest
        for i in candidates:
            extra = min(reach - holding[i], max(1, remaining * weights[i] // whole), rest)
            holding[i] = holding[i] + extra
            rest = rest - extra
    return np.array(holding)


def noise(key, shape, spread, most, shards=(), kind=jnp.bfloat16):
    array = jax.random.normal(key, shape, jnp.float32) * spread
    if len(shards) > 0:
        array = block_scale(key, shape, shards, -0.22, 0.18) * array
    return jnp.clip(array, min=-most, max=most).astype(kind)


def setup_inputs(seed: int = 0) -> dict:
    key_list = jax.random.split(jax.random.key(seed), 5)
    fmap1 = noise(key_list[0], (BATCH, H0, W0, C), 1.0, 6.0, ((1, 8), (2, 4)))
    fmap2 = noise(key_list[1], (BATCH, H0, W0, C), 1.0, 6.0, ((1, 8), (2, 4)))
    target_owner_keys = jax.random.split(jax.random.fold_in(key_list[2], 1), LEVELS * QBLK // QB_DEV)
    target_owner_turns = jax.random.permutation(jax.random.fold_in(key_list[2], 3), LEVELS * QBLK // QB_DEV)
    target_owner = jax.vmap(lambda own, number: routed_block(jax.random.fold_in(key_list[2], 2), own, number, QB_DEV, N_ROWS * N_COLS, 1, CAP, 2))(target_owner_keys, target_owner_turns).reshape((LEVELS, QBLK, 1))
    target_tile = with_ends(jax.random.randint(key_list[3], (LEVELS, QBLK), 0, TILES), jax.random.fold_in(key_list[3], 1), 0, TILES - 1).astype(jnp.int32)
    return dict(fmap1=fmap1, fmap2=fmap2, target_owner=target_owner, target_tile=target_tile)


def window_index():
    tile_side = 2 * RADIUS
    span_side = 4 * RADIUS
    window_side = 2 * RADIUS + 1
    query_ids = jnp.arange(tile_side * tile_side, dtype=jnp.int32)
    offset_ids = jnp.arange(window_side * window_side, dtype=jnp.int32)
    row_part = query_ids[:, None] // tile_side + offset_ids[None, :] // window_side
    col_part = query_ids[:, None] % tile_side + offset_ids[None, :] % window_side
    return row_part * span_side + col_part


def pool_level(level_map):
    frame_count, rows_in, cols_in, channels = level_map.shape
    pooled = level_map.astype(jnp.float32).reshape(frame_count, rows_in // 2, 2, cols_in // 2, 2, channels)
    return jnp.mean(pooled, axis=(2, 4)).astype(jnp.bfloat16)


def reference(fmap1, fmap2, target_owner, target_tile):
    tile_side = 2 * RADIUS
    span_side = 4 * RADIUS
    window_side = 2 * RADIUS + 1
    device_count = N_ROWS * N_COLS
    levels = [fmap2]
    for level in range(1, LEVELS):
        levels.append(pool_level(levels[-1]))
    padded = [jnp.pad(level_map, ((0, 0), (RADIUS, RADIUS), (RADIUS, RADIUS), (0, 0))) for level_map in levels]
    window_ids = window_index()
    tiles_across = QW // tile_side
    per_frame = (QH // tile_side) * tiles_across
    block_ids = jnp.arange(QB_DEV, dtype=jnp.int32)
    frame_ids = block_ids // per_frame
    block_rows = (block_ids % per_frame) // tiles_across * tile_side
    block_cols = block_ids % tiles_across * tile_side
    owner_table = target_owner[:, :, 0].reshape(LEVELS, device_count, QB_DEV)
    tile_table = target_tile.reshape(LEVELS, device_count, QB_DEV)
    gather_ids = jnp.broadcast_to(window_ids[None], (QB_DEV,) + window_ids.shape)

    def one_device(device):
        first_row = device // N_COLS * QH + block_rows
        first_col = device % N_COLS * QW + block_cols

        def query_block(frame_id, row_at, col_at):
            return lax.dynamic_slice(fmap1, (frame_id, row_at, col_at, 0 * frame_id), (1, tile_side, tile_side, C)).reshape(tile_side * tile_side, C)

        queries = jax.vmap(query_block)(frame_ids, first_row, first_col).astype(jnp.float32)
        results = []
        for level in range(LEVELS):
            level_rows = QH >> level
            level_cols = QW >> level
            level_across = level_cols // tile_side
            tile_count = (level_rows // tile_side) * level_across
            owner_ids = owner_table[level, device]
            tile_ids = tile_table[level, device] % tile_count
            target_rows = owner_ids // N_COLS * level_rows + tile_ids // level_across * tile_side
            target_cols = owner_ids % N_COLS * level_cols + tile_ids % level_across * tile_side

            def target_block(frame_id, row_at, col_at, source=padded[level]):
                return lax.dynamic_slice(source, (frame_id, row_at, col_at, 0 * frame_id), (1, span_side, span_side, C)).reshape(span_side * span_side, C)

            targets = jax.vmap(target_block)(frame_ids, target_rows, target_cols).astype(jnp.float32)
            scores = jnp.einsum("bqc,bpc->bqp", queries, targets, precision=lax.Precision.HIGHEST) * C ** -0.5
            results.append(jnp.take_along_axis(scores, gather_ids, axis=2))
        return jnp.stack(results)

    stacked = lax.map(one_device, jnp.arange(device_count, dtype=jnp.int32))
    return stacked.transpose(1, 4, 0, 2, 3).reshape(LEVELS, window_side * window_side, device_count * QB_DEV * tile_side * tile_side)
```

```python
import functools

import jax
import jax.numpy as jnp
from jax import lax
from jax.experimental import pallas as pl
from jax.experimental.pallas import tpu as pltpu
from jax.sharding import PartitionSpec as P

RADIUS = 4
LEVELS = 2


def padded_2(block, sides, width):
    for axis, dim in sides:
        count = lax.axis_size(axis)
        forward = [(i, i + 1) for i in range(count - 1)]
        backward = [(target, source) for source, target in forward]
        low = lax.ppermute(
            lax.slice_in_dim(block, block.shape[dim] - width, None, axis=dim), axis, forward
        )
        high = lax.ppermute(lax.slice_in_dim(block, 0, width, axis=dim), axis, backward)
        block = jnp.concatenate([low, block, high], axis=dim)
    return block


def pool_level(level_map):
    frame_count, rows_in, cols_in, channels = level_map.shape
    pooled = level_map.astype(jnp.float32).reshape(
        frame_count, rows_in // 2, 2, cols_in // 2, 2, channels
    )
    return jnp.mean(pooled, axis=(2, 4)).astype(jnp.bfloat16)


def dispatch_kernel(slot_count, block_ref, query_ref, sent_ref):
    base = pl.program_id(0) * slot_count
    for slot in range(slot_count):
        sent_ref[slot] = query_ref[block_ref[base + slot]]


def correlate_kernel(plan, scale, slot_count, label_ref, query_ref, *refs):
    map_refs, reply_ref = refs[:-1], refs[-1]
    per_frame, levels = plan
    tile_side = 2 * RADIUS
    span_side = 4 * RADIUS
    window_side = 2 * RADIUS + 1
    block_cells = tile_side * tile_side
    owner_slots = slot_count // LEVELS
    base = pl.program_id(0) * slot_count
    lane = lax.broadcasted_iota(jnp.int32, (1, 1, 2 * block_cells), 2)
    query_row = lane % block_cells // tile_side
    query_col = lane[0] % tile_side
    is_first = lane[0] < block_cells

    def window(slot):
        padded_rows, across = levels[slot // owner_slots]
        label = label_ref[base + slot]
        tile = label % per_frame
        row = label // per_frame * padded_rows + tile // across * tile_side
        col = pl.multiple_of(tile % across * tile_side, tile_side)
        cells = map_refs[slot // owner_slots][pl.ds(row, span_side), pl.ds(col, span_side), :]
        return cells.reshape(span_side * span_side, -1).astype(jnp.bfloat16)

    for pair in range(slot_count // 2):
        queries = query_ref[2 * pair : 2 * pair + 2].reshape(2 * block_cells, -1)
        first, second = [
            lax.dot_general(
                window(2 * pair + half),
                queries,
                (((1,), (1,)), ((), ())),
                preferred_element_type=jnp.float32,
            )
            for half in range(2)
        ]
        scores = jnp.where(is_first, first, second)
        scores = scores.reshape(span_side, span_side, 2 * block_cells)
        for bit in (1, 2, 4):
            scores = jnp.where((query_row & bit) != 0, scores[bit:], scores[:-bit])
        flat = scores.reshape(window_side * span_side, 2 * block_cells)
        for bit in (1, 2, 4):
            moved = pltpu.roll(flat, flat.shape[0] - bit, 0)
            flat = jnp.where((query_col & bit) != 0, moved, flat)
        flat = flat * scale
        for a in range(window_side):
            reply_ref[pair, a * window_side : (a + 1) * window_side, :] = flat[
                a * span_side : a * span_side + window_side
            ]


def assemble_kernel(pair_count, source_ref, half_ref, reply_ref, out_ref):
    lanes = reply_ref.shape[2]
    is_first = lax.broadcasted_iota(jnp.int32, reply_ref.shape[1:], 1) < lanes // 2
    for level in range(LEVELS):

        def step(m, carry, level=level):
            at = 2 * (level * pair_count + m)
            picked = []
            for side in range(2):
                rows = reply_ref[source_ref[at + side]]
                moved = pltpu.roll(rows, lanes // 2, 1)
                picked.append(jnp.where(half_ref[at + side] == side, rows, moved))
            spot = pl.ds(pl.multiple_of(m * lanes, lanes), lanes)
            out_ref[level, :, spot] = jnp.where(is_first, picked[0], picked[1])
            return carry

        lax.fori_loop(0, pair_count, step, 0)


def body(fmap1, fmap2, target_owner, target_tile):
    tile_side = 2 * RADIUS
    window_side = 2 * RADIUS + 1
    block_cells = tile_side * tile_side
    frame_count, band_rows, band_cols, channels = fmap1.shape
    device_count = lax.axis_size("rows") * lax.axis_size("cols")
    tiles_across = band_cols // tile_side
    per_frame = band_rows // tile_side * tiles_across
    block_count = frame_count * per_frame
    owner_slots = max(2, (2 * block_count + device_count - 1) // device_count)
    owner_slots += owner_slots % 2
    slot_count = LEVELS * owner_slots
    pair_slots = slot_count // 2
    queries = fmap1.reshape(
        frame_count, band_rows // tile_side, tile_side, tiles_across, tile_side, channels
    )
    queries = queries.transpose(0, 1, 3, 2, 4, 5).reshape(block_count, block_cells, channels)
    owner_ids = target_owner[:, :, 0]
    peer_ids = jnp.arange(device_count, dtype=jnp.int32)
    owner_hits = (owner_ids[:, :, None] == peer_ids[None, None, :]).astype(jnp.int32)
    slot_rank = jnp.sum(owner_hits * (jnp.cumsum(owner_hits, axis=1) - 1), axis=2)
    block_ids = jnp.arange(block_count, dtype=jnp.int32)
    label_rows = []
    for level in range(LEVELS):
        tile_count = (band_rows >> level) // tile_side * ((band_cols >> level) // tile_side)
        label_rows.append(block_ids // per_frame * per_frame + target_tile[level] % tile_count)
    rank_ids = jnp.arange(owner_slots, dtype=jnp.int32)
    rank_hits = (slot_rank[:, :, None] == rank_ids[None, None, :]).astype(jnp.int32)
    slot_hits = owner_hits[:, :, :, None] * rank_hits[:, :, None, :]

    def by_slot(values):
        table = jnp.sum(slot_hits * values[:, :, None, None], axis=1)
        return table.transpose(1, 0, 2).reshape(device_count, slot_count)

    labels_sent = by_slot(jnp.stack(label_rows))
    blocks_sent = by_slot(jnp.broadcast_to(block_ids[None], owner_ids.shape))
    slot_block = (slot_count, block_cells, channels)
    slot_total = device_count * slot_count
    queries_sent = pl.pallas_call(
        functools.partial(dispatch_kernel, slot_count),
        out_shape=jax.ShapeDtypeStruct((slot_total,) + slot_block[1:], jnp.bfloat16),
        grid_spec=pltpu.PrefetchScalarGridSpec(
            num_scalar_prefetch=1,
            grid=(device_count,),
            in_specs=[pl.BlockSpec(queries.shape, lambda d, *_: (0, 0, 0))],
            out_specs=pl.BlockSpec(slot_block, lambda d, *_: (d, 0, 0)),
        ),
    )(blocks_sent.reshape(-1), queries)
    label_part = lax.all_to_all(
        labels_sent, ("rows", "cols"), split_axis=0, concat_axis=0, tiled=True
    )
    query_part = lax.all_to_all(
        queries_sent.reshape((device_count,) + slot_block),
        ("rows", "cols"),
        split_axis=0,
        concat_axis=0,
        tiled=True,
    )
    levels = [fmap2]
    for level in range(1, LEVELS):
        levels.append(pool_level(levels[-1]))
    maps = []
    plan = []
    for level_map in levels:
        padded = padded_2(level_map, (("rows", 1), ("cols", 2)), RADIUS).astype(jnp.float32)
        maps.append(padded.reshape((-1,) + padded.shape[2:]))
        plan.append((padded.shape[1], level_map.shape[2] // tile_side))
    window_cells = window_side * window_side
    reply_block = (pair_slots, window_cells, 2 * block_cells)
    replies = pl.pallas_call(
        functools.partial(
            correlate_kernel, (per_frame, tuple(plan)), channels ** (-0.5), slot_count
        ),
        out_shape=jax.ShapeDtypeStruct(
            (device_count * pair_slots,) + reply_block[1:], jnp.float32
        ),
        grid_spec=pltpu.PrefetchScalarGridSpec(
            num_scalar_prefetch=1,
            grid=(device_count,),
            in_specs=[pl.BlockSpec(slot_block, lambda d, *_: (d, 0, 0))]
            + [pl.BlockSpec(level_map.shape, lambda d, *_: (0, 0, 0)) for level_map in maps],
            out_specs=pl.BlockSpec(reply_block, lambda d, *_: (d, 0, 0)),
        ),
    )(label_part.reshape(-1), query_part.reshape((slot_total,) + slot_block[1:]), *maps)
    returned = lax.all_to_all(
        replies.reshape((device_count,) + reply_block),
        ("rows", "cols"),
        split_axis=0,
        concat_axis=0,
        tiled=True,
    )
    level_ids = jnp.arange(LEVELS, dtype=jnp.int32)[:, None]
    slot_ids = level_ids * owner_slots + slot_rank
    source_ids = owner_ids * pair_slots + slot_ids // 2
    reply_table = returned.reshape((device_count * pair_slots,) + reply_block[1:])
    return pl.pallas_call(
        functools.partial(assemble_kernel, block_count // 2),
        out_shape=jax.ShapeDtypeStruct(
            (LEVELS, window_cells, block_count * block_cells), jnp.float32
        ),
        in_specs=[
            pl.BlockSpec(memory_space=pltpu.SMEM),
            pl.BlockSpec(memory_space=pltpu.SMEM),
            pl.BlockSpec(memory_space=pltpu.VMEM),
        ],
        out_specs=pl.BlockSpec(memory_space=pltpu.VMEM),
    )(source_ids.reshape(-1), (slot_ids % 2).reshape(-1), reply_table)


def solution(mesh):
    in_specs = (
        P(None, "rows", "cols", None),
        P(None, "rows", "cols", None),
        P(None, ("rows", "cols"), None),
        P(None, ("rows", "cols")),
    )
    out_specs = P(None, None, ("rows", "cols"))
    return jax.shard_map(body, mesh=mesh, in_specs=in_specs, out_specs=out_specs, check_vma=False)
```

```python
import functools

import jax
import jax.numpy as jnp
from jax import lax
from jax.experimental import pallas as pl
from jax.experimental.pallas import tpu as pltpu
from jax.sharding import PartitionSpec as P

RADIUS = 4
LEVELS = 2
STEP_SLOTS = 16


def padded_2(block, sides, width):
    for axis, dim in sides:
        count = lax.axis_size(axis)
        forward = [(i, i + 1) for i in range(count - 1)]
        backward = [(target, source) for source, target in forward]
        low = lax.ppermute(
            lax.slice_in_dim(block, block.shape[dim] - width, None, axis=dim), axis, forward
        )
        high = lax.ppermute(lax.slice_in_dim(block, 0, width, axis=dim), axis, backward)
        block = jnp.concatenate([low, block, high], axis=dim)
    return block


def pool_level(level_map):
    frame_count, rows_in, cols_in, channels = level_map.shape
    pooled = level_map.astype(jnp.float32).reshape(
        frame_count, rows_in // 2, 2, cols_in // 2, 2, channels
    )
    return jnp.mean(pooled, axis=(2, 4)).astype(jnp.bfloat16)


def dispatch_kernel(slot_count, block_ref, query_ref, sent_ref):
    base = pl.program_id(0) * slot_count
    for slot in range(slot_count):
        sent_ref[slot] = query_ref[block_ref[base + slot]]


def correlate_kernel(plan, scale, slot_count, label_ref, query_ref, *refs):
    map_refs, (reply_ref, held, arrived) = refs[:-3], refs[-3:]
    per_frame, col_count, levels = plan
    tile_side = 2 * RADIUS
    span_side = 4 * RADIUS
    window_side = 2 * RADIUS + 1
    block_cells = tile_side * tile_side
    step = pl.program_id(0)
    step_count = pl.num_programs(0)
    level_steps = slot_count // LEVELS // STEP_SLOTS
    lane = lax.broadcasted_iota(jnp.int32, (1, 1, 2 * block_cells), 2)
    query_row = lane % block_cells // tile_side
    query_col = lane[0] % tile_side
    is_first = lane[0] < block_cells

    def copy_of(at, slot, level):
        padded_rows, across = levels[level]
        label = label_ref[at * STEP_SLOTS + slot]
        tile = label % per_frame
        region = label // per_frame
        row = region // col_count * padded_rows + tile // across * tile_side
        col = (region % col_count * across + tile % across) * tile_side
        col = pl.multiple_of(col, tile_side)
        return pltpu.make_async_copy(
            map_refs[level].at[pl.ds(row, span_side), pl.ds(col, span_side), :],
            held.at[at % 2, slot],
            arrived.at[at % 2, slot],
        )

    def fetch(at):
        for level in range(LEVELS):

            @pl.when(at // level_steps % LEVELS == level)
            def _(level=level):
                for slot in range(STEP_SLOTS):
                    copy_of(at, slot, level).start()

    @pl.when(step == 0)
    def _():
        fetch(step)

    @pl.when(step + 1 < step_count)
    def _():
        fetch(step + 1)

    def window(slot):
        copy_of(step, slot, 0).wait()
        cells = held[step % 2, slot]
        return cells.reshape(span_side * span_side, -1).astype(jnp.bfloat16)

    for pair in range(STEP_SLOTS // 2):
        queries = query_ref[2 * pair : 2 * pair + 2].reshape(2 * block_cells, -1)
        first, second = [
            lax.dot_general(
                window(2 * pair + half),
                queries,
                (((1,), (1,)), ((), ())),
                preferred_element_type=jnp.float32,
            )
            for half in range(2)
        ]
        scores = jnp.where(is_first, first, second)
        scores = scores.reshape(span_side, span_side, 2 * block_cells)
        for bit in (1, 2, 4):
            scores = jnp.where((query_row & bit) != 0, scores[bit:], scores[:-bit])
        flat = scores.reshape(window_side * span_side, 2 * block_cells)
        for bit in (1, 2, 4):
            moved = pltpu.roll(flat, flat.shape[0] - bit, 0)
            flat = jnp.where((query_col & bit) != 0, moved, flat)
        flat = flat * scale
        for a in range(window_side):
            base = (pair * window_side + a) * window_side
            reply_ref[base : base + window_side, :] = flat[
                a * span_side : a * span_side + window_side
            ]


def assemble_kernel(pair_count, source_ref, half_ref, reply_ref, out_ref):
    window_cells, lanes = out_ref.shape[1], reply_ref.shape[1]
    is_first = lax.broadcasted_iota(jnp.int32, (window_cells, lanes), 1) < lanes // 2
    for level in range(LEVELS):

        def step(m, carry, level=level):
            at = 2 * (level * pair_count + m)
            picked = []
            for side in range(2):
                rows = reply_ref[pl.ds(source_ref[at + side] * window_cells, window_cells), :]
                moved = pltpu.roll(rows, lanes // 2, 1)
                picked.append(jnp.where(half_ref[at + side] == side, rows, moved))
            spot = pl.ds(pl.multiple_of(m * lanes, lanes), lanes)
            out_ref[level, :, spot] = jnp.where(is_first, picked[0], picked[1])
            return carry

        lax.fori_loop(0, pair_count, step, 0)


def body(fmap1, fmap2, target_owner, target_tile):
    tile_side = 2 * RADIUS
    window_side = 2 * RADIUS + 1
    block_cells = tile_side * tile_side
    frame_count, band_rows, band_cols, channels = fmap1.shape
    row_count = lax.axis_size("rows")
    col_count = lax.axis_size("cols")
    device_count = row_count * col_count
    tiles_across = band_cols // tile_side
    per_frame = band_rows // tile_side * tiles_across
    block_count = frame_count * per_frame
    owner_slots = max(2, (2 * block_count + device_count - 1) // device_count)
    row_slots = -(-owner_slots * col_count // STEP_SLOTS) * STEP_SLOTS
    slot_count = LEVELS * row_slots
    pair_slots = slot_count // 2
    queries = fmap1.reshape(
        frame_count, band_rows // tile_side, tile_side, tiles_across, tile_side, channels
    )
    queries = queries.transpose(0, 1, 3, 2, 4, 5).reshape(block_count, block_cells, channels)
    owner_ids = target_owner[:, :, 0]
    owner_rows = owner_ids // col_count
    peer_ids = jnp.arange(row_count, dtype=jnp.int32)
    owner_hits = (owner_rows[:, :, None] == peer_ids[None, None, :]).astype(jnp.int32)
    slot_rank = jnp.sum(owner_hits * (jnp.cumsum(owner_hits, axis=1) - 1), axis=2)
    block_ids = jnp.arange(block_count, dtype=jnp.int32)
    label_rows = []
    for level in range(LEVELS):
        tile_count = (band_rows >> level) // tile_side * ((band_cols >> level) // tile_side)
        regions = block_ids // per_frame * col_count + owner_ids[level] % col_count
        label_rows.append(regions * per_frame + target_tile[level] % tile_count)
    rank_ids = jnp.arange(row_slots, dtype=jnp.int32)
    rank_hits = (slot_rank[:, :, None] == rank_ids[None, None, :]).astype(jnp.int32)
    slot_hits = owner_hits[:, :, :, None] * rank_hits[:, :, None, :]

    def by_slot(values):
        table = jnp.sum(slot_hits * values[:, :, None, None], axis=1)
        return table.transpose(1, 0, 2).reshape(row_count, slot_count)

    labels_sent = by_slot(jnp.stack(label_rows))
    blocks_sent = by_slot(jnp.broadcast_to(block_ids[None], owner_ids.shape))
    slot_block = (slot_count, block_cells, channels)
    slot_total = row_count * slot_count
    queries_sent = pl.pallas_call(
        functools.partial(dispatch_kernel, slot_count),
        out_shape=jax.ShapeDtypeStruct((slot_total,) + slot_block[1:], jnp.bfloat16),
        grid_spec=pltpu.PrefetchScalarGridSpec(
            num_scalar_prefetch=1,
            grid=(row_count,),
            in_specs=[pl.BlockSpec(queries.shape, lambda d, *_: (0, 0, 0))],
            out_specs=pl.BlockSpec(slot_block, lambda d, *_: (d, 0, 0)),
        ),
    )(blocks_sent.reshape(-1), queries)
    label_part = lax.all_to_all(
        labels_sent, "rows", split_axis=0, concat_axis=0, tiled=True
    )
    query_part = lax.all_to_all(
        queries_sent.reshape((row_count,) + slot_block),
        "rows",
        split_axis=0,
        concat_axis=0,
        tiled=True,
    )
    levels = [fmap2]
    for level in range(1, LEVELS):
        levels.append(pool_level(levels[-1]))
    maps = []
    plan = []
    for level_map in levels:
        across = level_map.shape[2] // tile_side
        band = lax.all_gather(level_map, "cols", axis=2, tiled=True)
        padded = padded_2(band, (("rows", 1),), RADIUS).astype(jnp.float32)
        padded = jnp.pad(padded, ((0, 0), (0, 0), (RADIUS, RADIUS), (0, 0)))
        maps.append(padded.reshape((-1,) + padded.shape[2:]))
        plan.append((padded.shape[1], across))
    window_cells = window_side * window_side
    span_side = 4 * RADIUS
    step_block = (STEP_SLOTS, block_cells, channels)
    reply_block = (STEP_SLOTS // 2 * window_cells, 2 * block_cells)
    replies = pl.pallas_call(
        functools.partial(
            correlate_kernel,
            (per_frame, col_count, tuple(plan)),
            channels ** (-0.5),
            slot_count,
        ),
        out_shape=jax.ShapeDtypeStruct(
            (row_count * pair_slots * window_cells, 2 * block_cells), jnp.float32
        ),
        grid_spec=pltpu.PrefetchScalarGridSpec(
            num_scalar_prefetch=1,
            grid=(slot_total // STEP_SLOTS,),
            in_specs=[pl.BlockSpec(step_block, lambda d, *_: (d, 0, 0))]
            + [pl.BlockSpec(memory_space=pltpu.HBM)] * LEVELS,
            out_specs=pl.BlockSpec(reply_block, lambda d, *_: (d, 0)),
            scratch_shapes=[
                pltpu.VMEM((2, STEP_SLOTS, span_side, span_side, channels), jnp.float32),
                pltpu.SemaphoreType.DMA((2, STEP_SLOTS)),
            ],
        ),
    )(label_part.reshape(-1), query_part.reshape((slot_total,) + slot_block[1:]), *maps)
    returned = lax.all_to_all(
        replies.reshape(row_count, pair_slots * window_cells, 2 * block_cells),
        "rows",
        split_axis=0,
        concat_axis=0,
        tiled=True,
    )
    level_ids = jnp.arange(LEVELS, dtype=jnp.int32)[:, None]
    slot_ids = level_ids * row_slots + slot_rank
    source_ids = owner_rows * pair_slots + slot_ids // 2
    reply_table = returned.reshape(-1, 2 * block_cells)
    return pl.pallas_call(
        functools.partial(assemble_kernel, block_count // 2),
        out_shape=jax.ShapeDtypeStruct(
            (LEVELS, window_cells, block_count * block_cells), jnp.float32
        ),
        in_specs=[
            pl.BlockSpec(memory_space=pltpu.SMEM),
            pl.BlockSpec(memory_space=pltpu.SMEM),
            pl.BlockSpec(memory_space=pltpu.VMEM),
        ],
        out_specs=pl.BlockSpec(memory_space=pltpu.VMEM),
    )(source_ids.reshape(-1), (slot_ids % 2).reshape(-1), reply_table)


def solution(mesh):
    in_specs = (
        P(None, "rows", "cols", None),
        P(None, "rows", "cols", None),
        P(None, ("rows", "cols"), None),
        P(None, ("rows", "cols")),
    )
    out_specs = P(None, None, ("rows", "cols"))
    return jax.shard_map(body, mesh=mesh, in_specs=in_specs, out_specs=out_specs, check_vma=False)
```

```python
import functools

import jax
import jax.numpy as jnp
from jax import lax
from jax.experimental import pallas as pl
from jax.experimental.pallas import tpu as pltpu
from jax.sharding import PartitionSpec as P

RADIUS = 4
LEVELS = 2
STEP_SLOTS = 16


def padded_2(block, sides, width):
    for axis, dim in sides:
        count = lax.axis_size(axis)
        forward = [(i, i + 1) for i in range(count - 1)]
        backward = [(target, source) for source, target in forward]
        low = lax.ppermute(
            lax.slice_in_dim(block, block.shape[dim] - width, None, axis=dim), axis, forward
        )
        high = lax.ppermute(lax.slice_in_dim(block, 0, width, axis=dim), axis, backward)
        block = jnp.concatenate([low, block, high], axis=dim)
    return block


def pool_level(level_map):
    frame_count, rows_in, cols_in, channels = level_map.shape
    pooled = level_map.astype(jnp.float32).reshape(
        frame_count, rows_in // 2, 2, cols_in // 2, 2, channels
    )
    return jnp.mean(pooled, axis=(2, 4)).astype(jnp.bfloat16)


def dispatch_kernel(slot_count, block_ref, query_ref, sent_ref):
    base = pl.program_id(0) * slot_count
    for slot in range(slot_count):
        sent_ref[slot] = query_ref[block_ref[base + slot]]


def correlate_kernel(plan, scale, label_ref, query_ref, map_ref, reply_ref):
    per_frame, col_count, padded_rows, across = plan
    tile_side = 2 * RADIUS
    span_side = 4 * RADIUS
    window_side = 2 * RADIUS + 1
    block_cells = tile_side * tile_side
    base = pl.program_id(0) * STEP_SLOTS
    lane = lax.broadcasted_iota(jnp.int32, (1, 1, 2 * block_cells), 2)
    query_row = lane % block_cells // tile_side
    query_col = lane[0] % tile_side
    is_first = lane[0] < block_cells

    def window(slot):
        label = label_ref[base + slot]
        tile = label % per_frame
        region = label // per_frame
        row = region // col_count * padded_rows + tile // across * tile_side
        col = (region % col_count * across + tile % across) * tile_side
        col = pl.multiple_of(col, tile_side)
        cells = map_ref[pl.ds(row, span_side), pl.ds(col, span_side), :]
        return cells.reshape(span_side * span_side, -1).astype(jnp.bfloat16)

    for pair in range(STEP_SLOTS // 2):
        queries = query_ref[2 * pair : 2 * pair + 2].reshape(2 * block_cells, -1)
        first, second = [
            lax.dot_general(
                window(2 * pair + half),
                queries,
                (((1,), (1,)), ((), ())),
                preferred_element_type=jnp.float32,
            )
            for half in range(2)
        ]
        scores = jnp.where(is_first, first, second)
        scores = scores.reshape(span_side, span_side, 2 * block_cells)
        for bit in (1, 2, 4):
            scores = jnp.where((query_row & bit) != 0, scores[bit:], scores[:-bit])
        flat = scores.reshape(window_side * span_side, 2 * block_cells)
        for bit in (1, 2, 4):
            moved = pltpu.roll(flat, flat.shape[0] - bit, 0)
            flat = jnp.where((query_col & bit) != 0, moved, flat)
        flat = flat * scale
        for a in range(window_side):
            at = (pair * window_side + a) * window_side
            reply_ref[at : at + window_side, :] = flat[
                a * span_side : a * span_side + window_side
            ]


def assemble_kernel(pair_count, source_ref, half_ref, *refs):
    reply_refs, out_ref = refs[:-1], refs[-1]
    window_cells, lanes = out_ref.shape[1], reply_refs[0].shape[1]
    is_first = lax.broadcasted_iota(jnp.int32, (window_cells, lanes), 1) < lanes // 2
    for level in range(LEVELS):

        def step(m, carry, level=level):
            at = 2 * (level * pair_count + m)
            picked = []
            for side in range(2):
                first_row = source_ref[at + side] * window_cells
                rows = reply_refs[level][pl.ds(first_row, window_cells), :]
                moved = pltpu.roll(rows, lanes // 2, 1)
                picked.append(jnp.where(half_ref[at + side] == side, rows, moved))
            spot = pl.ds(pl.multiple_of(m * lanes, lanes), lanes)
            out_ref[level, :, spot] = jnp.where(is_first, picked[0], picked[1])
            return carry

        lax.fori_loop(0, pair_count, step, 0)


def body(fmap1, fmap2, target_owner, target_tile):
    tile_side = 2 * RADIUS
    window_side = 2 * RADIUS + 1
    block_cells = tile_side * tile_side
    frame_count, band_rows, band_cols, channels = fmap1.shape
    row_count = lax.axis_size("rows")
    col_count = lax.axis_size("cols")
    device_count = row_count * col_count
    tiles_across = band_cols // tile_side
    per_frame = band_rows // tile_side * tiles_across
    block_count = frame_count * per_frame
    owner_slots = max(2, (2 * block_count + device_count - 1) // device_count)
    row_slots = -(-owner_slots * col_count // STEP_SLOTS) * STEP_SLOTS
    pair_slots = row_slots // 2
    queries = fmap1.reshape(
        frame_count, band_rows // tile_side, tile_side, tiles_across, tile_side, channels
    )
    queries = queries.transpose(0, 1, 3, 2, 4, 5).reshape(block_count, block_cells, channels)
    owner_ids = target_owner[:, :, 0]
    owner_rows = owner_ids // col_count
    peer_ids = jnp.arange(row_count, dtype=jnp.int32)
    owner_hits = (owner_rows[:, :, None] == peer_ids[None, None, :]).astype(jnp.int32)
    slot_rank = jnp.sum(owner_hits * (jnp.cumsum(owner_hits, axis=1) - 1), axis=2)
    block_ids = jnp.arange(block_count, dtype=jnp.int32)
    label_rows = []
    for level in range(LEVELS):
        tile_count = (band_rows >> level) // tile_side * ((band_cols >> level) // tile_side)
        regions = block_ids // per_frame * col_count + owner_ids[level] % col_count
        label_rows.append(regions * per_frame + target_tile[level] % tile_count)
    rank_ids = jnp.arange(row_slots, dtype=jnp.int32)
    rank_hits = (slot_rank[:, :, None] == rank_ids[None, None, :]).astype(jnp.int32)
    slot_hits = owner_hits[:, :, :, None] * rank_hits[:, :, None, :]

    def by_slot(values):
        table = jnp.sum(slot_hits * values[:, :, None, None], axis=1)
        return table.transpose(1, 0, 2)

    labels_sent = by_slot(jnp.stack(label_rows))
    blocks_sent = by_slot(jnp.broadcast_to(block_ids[None], owner_ids.shape))
    slot_block = (row_slots, block_cells, channels)
    slot_total = row_count * row_slots
    label_part = lax.all_to_all(labels_sent, "rows", split_axis=0, concat_axis=0, tiled=True)
    levels = [fmap2]
    for level in range(1, LEVELS):
        levels.append(pool_level(levels[-1]))
    window_cells = window_side * window_side
    step_block = (STEP_SLOTS, block_cells, channels)
    reply_block = (STEP_SLOTS // 2 * window_cells, 2 * block_cells)
    reply_tables = [None] * LEVELS
    earlier = None
    for level in reversed(range(LEVELS)):
        queries_sent = pl.pallas_call(
            functools.partial(dispatch_kernel, row_slots),
            out_shape=jax.ShapeDtypeStruct((slot_total,) + slot_block[1:], jnp.bfloat16),
            grid_spec=pltpu.PrefetchScalarGridSpec(
                num_scalar_prefetch=1,
                grid=(row_count,),
                in_specs=[pl.BlockSpec(queries.shape, lambda d, *_: (0, 0, 0))],
                out_specs=pl.BlockSpec(slot_block, lambda d, *_: (d, 0, 0)),
            ),
        )(blocks_sent[:, level].reshape(-1), queries)
        query_part = lax.all_to_all(
            queries_sent.reshape((row_count,) + slot_block),
            "rows",
            split_axis=0,
            concat_axis=0,
            tiled=True,
        )
        band = lax.all_gather(levels[level], "cols", axis=2, tiled=True)
        if earlier is not None:
            band = lax.optimization_barrier((band, earlier))[0]
        padded = padded_2(band, (("rows", 1),), RADIUS).astype(jnp.float32)
        padded = jnp.pad(padded, ((0, 0), (0, 0), (RADIUS, RADIUS), (0, 0)))
        level_map = padded.reshape((-1,) + padded.shape[2:])
        plan = (per_frame, col_count, padded.shape[1], levels[level].shape[2] // tile_side)
        replies = pl.pallas_call(
            functools.partial(correlate_kernel, plan, channels ** (-0.5)),
            out_shape=jax.ShapeDtypeStruct(
                (row_count * pair_slots * window_cells, 2 * block_cells), jnp.float32
            ),
            grid_spec=pltpu.PrefetchScalarGridSpec(
                num_scalar_prefetch=1,
                grid=(slot_total // STEP_SLOTS,),
                in_specs=[
                    pl.BlockSpec(step_block, lambda d, *_: (d, 0, 0)),
                    pl.BlockSpec(
                        level_map.shape, lambda d, *_: (0, 0, 0), pipeline_mode=pl.Buffered(1)
                    ),
                ],
                out_specs=pl.BlockSpec(reply_block, lambda d, *_: (d, 0)),
            ),
        )(
            label_part[:, level].reshape(-1),
            query_part.reshape((slot_total,) + slot_block[1:]),
            level_map,
        )
        returned = lax.all_to_all(
            replies.reshape(row_count, pair_slots * window_cells, 2 * block_cells),
            "rows",
            split_axis=0,
            concat_axis=0,
            tiled=True,
        )
        earlier = returned
        reply_tables[level] = returned.reshape(-1, 2 * block_cells)
    source_ids = owner_rows * pair_slots + slot_rank // 2
    return pl.pallas_call(
        functools.partial(assemble_kernel, block_count // 2),
        out_shape=jax.ShapeDtypeStruct(
            (LEVELS, window_cells, block_count * block_cells), jnp.float32
        ),
        in_specs=[
            pl.BlockSpec(memory_space=pltpu.SMEM),
            pl.BlockSpec(memory_space=pltpu.SMEM),
        ]
        + [pl.BlockSpec(memory_space=pltpu.VMEM)] * LEVELS,
        out_specs=pl.BlockSpec(memory_space=pltpu.VMEM),
    )(source_ids.reshape(-1), (slot_rank % 2).reshape(-1), *reply_tables)


def solution(mesh):
    in_specs = (
        P(None, "rows", "cols", None),
        P(None, "rows", "cols", None),
        P(None, ("rows", "cols"), None),
        P(None, ("rows", "cols")),
    )
    out_specs = P(None, None, ("rows", "cols"))
    return jax.shard_map(body, mesh=mesh, in_specs=in_specs, out_specs=out_specs, check_vma=False)
```
